32 devices in a mesh: items: 4 (over y, x), users: 8 (over z, core).
Axes of the slice: x: 2, y: 2, z: 4, core: 2. Of those that a mesh axis runs over, the one named last changes fastest.
Arguments:
- capsules: bfloat16 [512, 8, 128], P('users'), may hold values from -6 to 6
- bank: bfloat16 [32768, 128], P(('items', 'users')), may hold values from -0.5 to 0.5
Outputs:
- relative: float32 [512, 32], P('users', 'items')
- peak: float32 [512], P('users')
The draws below stay inside these ranges and needn't reach their ends.
All inputs are finite; a program needn't handle non-finite values.
Results may differ from the reference program's by a relative error of at most 0.0003.
Values may be sent and summed in bfloat16 or wider, within the bound.
A program may use at most 64 MiB of HBM per device.

```python
import jax
import jax.numpy as jnp
from jax import lax

E = 128
K = 8
BLOCK = 1024
USERS = 512
NB = 32
NITEMS = 32768


def block_levels(key, shape, split, least, largest):
    gain, own = 1.0, jax.random.fold_in(key, 6)
    for axis_at, shards_of in split:
        steps = jnp.exp(jax.random.uniform(jax.random.fold_in(own, axis_at), (shards_of,), jnp.float32, least / len(split), largest / len(split)))
        gain = gain * jnp.repeat(steps, shape[axis_at] // shards_of).reshape([-1 if axis == axis_at else 1 for axis in range(len(shape))])
    return gain


def normal_values(key, shape, scale, limit, split=(), kind=jnp.bfloat16):
    array = scale * jax.random.normal(key, shape, jnp.float32)
    if split:
        array = array * block_levels(key, shape, split, -0.22, 0.18)
    return jnp.clip(array, -limit, limit).astype(kind)


def setup_inputs(seed: int = 0) -> dict:
    streams_of = jax.random.split(jax.random.key(seed), 3)
    capsules = normal_values(streams_of[0], (USERS, K, E), 1.0, 6.0, ((0, 8),))
    bank = normal_values(streams_of[1], (NITEMS, E), E ** -0.5, 0.5, ((0, 32),))
    return {"capsules": capsules, "bank": bank}


def reference(capsules, bank):
    flat = capsules.reshape(USERS * K, E)
    blocks = bank.reshape(NB, BLOCK, E)

    def one_block(rows):
        score = jnp.dot(flat, rows.T, preferred_element_type=jnp.float32)
        return jnp.max(score.reshape(USERS, K * BLOCK), axis=1)

    block_peak = lax.map(one_block, blocks).T
    peak = jnp.max(block_peak, axis=1)
    return block_peak - peak[:, None], peak
```

```python
import functools

import jax
import jax.numpy as jnp
from jax import lax
from jax.experimental import pallas as pl
from jax.experimental.pallas import tpu as pltpu
from jax.sharding import PartitionSpec as P

BLOCK = 1024
LANES = 128
MESH = pl.DeviceIdType.MESH


def landed(ref, sem):
    pltpu.make_async_copy(ref, ref, sem).wait()


def partner_line(z, d, count):
    if count & (count - 1):
        return (z + d) % count
    out, bit = 0, 1
    while bit < count:
        out = out + ((z // bit + d // bit) % 2) * bit
        bit *= 2
    return out


def fold_capsules(acc):
    tiles = acc.shape[1] // LANES
    lane = lax.broadcasted_iota(jnp.int32, (8, LANES), 1) % 8
    out = None
    for t in range(tiles):
        v = acc[:, t * LANES : (t + 1) * LANES]
        for shift in (1, 2, 4):
            v = jnp.maximum(v, pltpu.roll(v, LANES - shift, 1))
        v = v if t == 0 else pltpu.roll(v, t, 1)
        out = v if out is None else jnp.where(lane == t, v, out)
    return jnp.max(out, axis=0, keepdims=True)


def kernel(
    items, users, caps_hbm, bank_hbm, rel_ref, peak_ref,
    own, bank, all_caps, res, table,
    load_sem, send_sem, recv_sem, back_send, back_recv,
):
    i = lax.axis_index("items")
    g = lax.axis_index("users")
    chips = users // 2
    z, c = g // 2, g % 2
    p = 2 * z + 1 - c
    pieces, rows = all_caps.shape[1], all_caps.shape[2]

    load_caps = pltpu.make_async_copy(caps_hbm, own, load_sem.at[0])
    load_caps.start()
    load_bank = pltpu.make_async_copy(bank_hbm, bank, load_sem.at[1])
    load_bank.start()

    barrier = pltpu.get_barrier_semaphore()

    def hello(jj, gg):
        pl.semaphore_signal(
            barrier, inc=1, device_id={"items": jj, "users": gg}, device_id_type=MESH
        )

    def hello_line(d, carry):
        hello(i, 2 * partner_line(z, d, chips) + c)
        return carry

    lax.fori_loop(1, chips, hello_line, 0, unroll=chips <= 8)
    for d in range(1, items):
        hello((i + d) % items, g)
    hello(i, p)
    pl.semaphore_wait(barrier, chips - 1 + items - 1 + 1)
    load_caps.wait()

    def send(src, dst, recv, jj, gg):
        pltpu.make_async_remote_copy(
            src_ref=src, dst_ref=dst, send_sem=send_sem.at[0], recv_sem=recv,
            device_id={"items": jj, "users": gg}, device_id_type=MESH,
        ).start()

    def send_line(d, carry):
        far = partner_line(z, chips - d, chips)
        send(own.at[i], all_caps.at[g, i], recv_sem.at[g, i], i, 2 * far + c)
        return carry

    lax.fori_loop(1, chips, send_line, 0, unroll=chips <= 8)
    send(own, all_caps.at[g], recv_sem.at[g, 0], i, p)
    load_bank.wait()

    def block_peak(group):
        score = lax.dot_general(
            bank[...], group.reshape(pieces * rows, group.shape[-1]),
            (((1,), (1,)), ((), ())), preferred_element_type=jnp.float32,
        )
        acc = jnp.max(score.reshape(-1, 8, pieces * rows), axis=0)
        return fold_capsules(acc)

    def answer(gg, jj):
        row = ((i - jj + items) % items) * users + g
        pltpu.make_async_remote_copy(
            src_ref=res.at[gg], dst_ref=table.at[row],
            send_sem=back_send.at[0], recv_sem=back_recv.at[0],
            device_id={"items": jj, "users": gg}, device_id_type=MESH,
        ).start()

    table[g] = block_peak(own[...])
    res[g] = table[g]

    def relay(d, carry):
        from_g = 2 * partner_line(z, d, chips) + c
        piece, sem = all_caps.at[from_g, i], recv_sem.at[from_g, i]
        landed(piece, sem)
        for s in range(1, items):
            send(piece, piece, sem, (i + s) % items, g)
        send(piece, piece, sem, i, p)
        return carry

    lax.fori_loop(1, chips, relay, 0, unroll=chips <= 8)
    landed(all_caps.at[p], recv_sem.at[p, 0])
    res[p] = block_peak(all_caps[p])

    def same_core(d, carry):
        from_g = 2 * partner_line(z, d, chips) + c
        for s in range(1, items):
            q = (i + s) % items
            piece, sem = all_caps.at[from_g, q], recv_sem.at[from_g, q]
            landed(piece, sem)
            send(piece, piece, sem, i, p)
        res[from_g] = block_peak(all_caps[from_g])
        for s in range(items):
            answer(from_g, (i + s) % items)
        return carry

    lax.fori_loop(1, chips, same_core, 0)

    def other_core(d, carry):
        from_g = 2 * partner_line(z, d, chips) + 1 - c
        for q in range(items):
            landed(all_caps.at[from_g, q], recv_sem.at[from_g, q])
        res[from_g] = block_peak(all_caps[from_g])
        for s in range(items):
            answer(from_g, (i + s) % items)
        return carry

    lax.fori_loop(1, chips, other_core, 0)
    for s in range(items):
        answer(p, (i + s) % items)
    for s in range(1, items):
        answer(g, (i + s) % items)

    blocks = items * users
    landed(table.at[pl.ds(0, blocks - 1)], back_recv.at[0])
    peak = jnp.max(table[...], axis=0)
    both = jnp.concatenate([table[:users].reshape(users, LANES) - peak, peak], axis=0)
    tiles = pieces * rows // LANES
    spread = LANES // 8
    lane = lax.broadcasted_iota(jnp.int32, both.shape, 1)
    pick = (lane % spread) * 8 + lane // spread
    both = jnp.take_along_axis(both, pick, axis=1)
    rel_ref[...] = both[:users, : tiles * spread]
    peak_ref[...] = both[users:, : tiles * spread]

    landed(all_caps.at[pl.ds(0, users - 1)], send_sem.at[0])
    landed(table.at[pl.ds(0, blocks - 1)], back_send.at[0])


def per_device(items, users, capsules, bank):
    users_here, k, width = capsules.shape
    assert k == 8 and bank.shape[0] == BLOCK and users_here * k <= 8 * LANES
    rows = users_here * k // items
    blocks = items * users
    relative, peak = pl.pallas_call(
        functools.partial(kernel, items, users),
        out_shape=(
            jax.ShapeDtypeStruct((users, users_here), jnp.float32),
            jax.ShapeDtypeStruct((1, users_here), jnp.float32),
        ),
        in_specs=[pl.BlockSpec(memory_space=pl.ANY)] * 2,
        out_specs=(pl.BlockSpec(memory_space=pltpu.VMEM),) * 2,
        scratch_shapes=[
            pltpu.VMEM((items, rows, width), capsules.dtype),
            pltpu.VMEM(bank.shape, bank.dtype),
            pltpu.VMEM((users, items, rows, width), capsules.dtype),
            pltpu.VMEM((users, 1, LANES), jnp.float32),
            pltpu.VMEM((blocks, 1, LANES), jnp.float32),
            pltpu.SemaphoreType.DMA((2,)),
            pltpu.SemaphoreType.DMA((1,)),
            pltpu.SemaphoreType.DMA((users, items)),
            pltpu.SemaphoreType.DMA((1,)),
            pltpu.SemaphoreType.DMA((1,)),
        ],
        compiler_params=pltpu.CompilerParams(
            collective_id=0, has_side_effects=True, vmem_limit_bytes=60 * 2**20
        ),
    )(capsules.reshape(items, rows, width), bank)
    return relative.T, peak.reshape(users_here)


def solution(mesh):
    return jax.shard_map(
        functools.partial(per_device, mesh.shape["items"], mesh.shape["users"]),
        mesh=mesh,
        in_specs=(P("users", None, None), P(("items", "users"), None)),
        out_specs=(P("users", "items"), P("users")),
        check_vma=False,
    )
```

```python
import functools

import jax
import jax.numpy as jnp
from jax import lax
from jax.experimental import pallas as pl
from jax.experimental.pallas import tpu as pltpu
from jax.sharding import PartitionSpec as P

BLOCK = 1024
LANES = 128
MESH = pl.DeviceIdType.MESH


def landed(ref, sem):
    pltpu.make_async_copy(ref, ref, sem).wait()


def partner_line(z, d, count):
    if count & (count - 1):
        return (z + d) % count
    out, bit = 0, 1
    while bit < count:
        out = out + ((z // bit + d // bit) % 2) * bit
        bit *= 2
    return out


def by_user(top):
    spread = LANES // 8
    lane = lax.broadcasted_iota(jnp.int32, (top.shape[0], LANES), 1)
    out = None
    for t in range(top.shape[1] // LANES):
        v = top[:, t * LANES : (t + 1) * LANES]
        for shift in (1, 2, 4):
            v = jnp.maximum(v, pltpu.roll(v, LANES - shift, 1))
        v = jnp.take_along_axis(v, (lane % spread) * 8, axis=1)
        out = v if out is None else jnp.where(lane // spread == t, v, out)
    return out


def kernel(
    items, users, caps_hbm, bank_hbm, rel_ref, peak_ref,
    own, bank, all_caps, res, table,
    load_sem, send_sem, recv_sem, back_send, back_recv,
):
    i = lax.axis_index("items")
    g = lax.axis_index("users")
    chips = users // 2
    z, c = g // 2, g % 2
    p = 2 * z + 1 - c
    pieces, rows = all_caps.shape[1], all_caps.shape[2]

    load_caps = pltpu.make_async_copy(caps_hbm, own, load_sem.at[0])
    load_caps.start()
    load_bank = pltpu.make_async_copy(bank_hbm, bank, load_sem.at[1])
    load_bank.start()

    barrier = pltpu.get_barrier_semaphore()

    def hello(jj, gg):
        pl.semaphore_signal(
            barrier, inc=1, device_id={"items": jj, "users": gg}, device_id_type=MESH
        )

    def hello_line(d, carry):
        hello(i, 2 * partner_line(z, d, chips) + c)
        return carry

    lax.fori_loop(1, chips, hello_line, 0, unroll=chips <= 8)
    for d in range(1, items):
        hello((i + d) % items, g)
    hello(i, p)
    pl.semaphore_wait(barrier, chips - 1 + items - 1 + 1)
    load_caps.wait()

    def send(src, dst, recv, jj, gg):
        pltpu.make_async_remote_copy(
            src_ref=src, dst_ref=dst, send_sem=send_sem.at[0], recv_sem=recv,
            device_id={"items": jj, "users": gg}, device_id_type=MESH,
        ).start()

    def send_line(d, carry):
        far = partner_line(z, chips - d, chips)
        send(own.at[i], all_caps.at[g, i], recv_sem.at[g, i], i, 2 * far + c)
        return carry

    lax.fori_loop(1, chips, send_line, 0, unroll=chips <= 8)
    send(own, all_caps.at[g], recv_sem.at[g, 0], i, p)
    load_bank.wait()

    def block_peak(group):
        score = lax.dot_general(
            bank[...], group.reshape(pieces * rows, group.shape[-1]),
            (((1,), (1,)), ((), ())), preferred_element_type=jnp.float32,
        )
        return jnp.max(score, axis=0, keepdims=True)

    def answer(gg, jj):
        row = ((i - jj + items) % items) * users + g
        pltpu.make_async_remote_copy(
            src_ref=res.at[gg], dst_ref=table.at[row],
            send_sem=back_send.at[0], recv_sem=back_recv.at[0],
            device_id={"items": jj, "users": gg}, device_id_type=MESH,
        ).start()

    table[g] = block_peak(own[...])
    res[g] = table[g]

    def relay(d, carry):
        from_g = 2 * partner_line(z, d, chips) + c
        piece, sem = all_caps.at[from_g, i], recv_sem.at[from_g, i]
        landed(piece, sem)
        for s in range(1, items):
            send(piece, piece, sem, (i + s) % items, g)
        send(piece, piece, sem, i, p)
        return carry

    lax.fori_loop(1, chips, relay, 0, unroll=chips <= 8)
    landed(all_caps.at[p], recv_sem.at[p, 0])
    res[p] = block_peak(all_caps[p])

    def same_core(d, carry):
        from_g = 2 * partner_line(z, d, chips) + c
        for s in range(1, items):
            q = (i + s) % items
            piece, sem = all_caps.at[from_g, q], recv_sem.at[from_g, q]
            landed(piece, sem)
            send(piece, piece, sem, i, p)
        res[from_g] = block_peak(all_caps[from_g])
        for s in range(items):
            answer(from_g, (i + s) % items)
        return carry

    lax.fori_loop(1, chips, same_core, 0)

    def other_core(d, carry):
        from_g = 2 * partner_line(z, d, chips) + 1 - c
        for q in range(items):
            landed(all_caps.at[from_g, q], recv_sem.at[from_g, q])
        res[from_g] = block_peak(all_caps[from_g])
        for s in range(items):
            answer(from_g, (i + s) % items)
        return carry

    lax.fori_loop(1, chips, other_core, 0)
    for s in range(items):
        answer(p, (i + s) % items)
    for s in range(1, items):
        answer(g, (i + s) % items)

    blocks = items * users
    landed(table.at[pl.ds(0, blocks - 1)], back_recv.at[0])
    best = jnp.max(table[...], axis=0)
    near = table[:users].reshape(users, best.shape[1])
    both = by_user(jnp.concatenate([near, best], axis=0))[:, : peak_ref.shape[1]]
    rel_ref[...] = both[:users] - both[users:]
    peak_ref[...] = both[users:]

    landed(all_caps.at[pl.ds(0, users - 1)], send_sem.at[0])
    landed(table.at[pl.ds(0, blocks - 1)], back_send.at[0])


def per_device(items, users, capsules, bank):
    users_here, k, width = capsules.shape
    assert k == 8 and bank.shape[0] == BLOCK and users_here * k <= 8 * LANES
    rows = users_here * k // items
    blocks = items * users
    relative, peak = pl.pallas_call(
        functools.partial(kernel, items, users),
        out_shape=(
            pltpu.VMEM((users, users_here), jnp.float32),
            pltpu.VMEM((1, users_here), jnp.float32),
        ),
        in_specs=[pl.BlockSpec(memory_space=pltpu.HBM)] * 2,
        out_specs=(pl.BlockSpec(memory_space=pltpu.VMEM),) * 2,
        scratch_shapes=[
            pltpu.VMEM((items, rows, width), capsules.dtype),
            pltpu.VMEM(bank.shape, bank.dtype),
            pltpu.VMEM((users, items, rows, width), capsules.dtype),
            pltpu.VMEM((users, 1, users_here * k), jnp.float32),
            pltpu.VMEM((blocks, 1, users_here * k), jnp.float32),
            pltpu.SemaphoreType.DMA((2,)),
            pltpu.SemaphoreType.DMA((1,)),
            pltpu.SemaphoreType.DMA((users, items)),
            pltpu.SemaphoreType.DMA((1,)),
            pltpu.SemaphoreType.DMA((1,)),
        ],
        compiler_params=pltpu.CompilerParams(
            collective_id=0, has_side_effects=True, vmem_limit_bytes=60 * 2**20
        ),
    )(capsules.reshape(items, rows, width), bank)
    return relative.T, peak.reshape(users_here)


def solution(mesh):
    return jax.shard_map(
        functools.partial(per_device, mesh.shape["items"], mesh.shape["users"]),
        mesh=mesh,
        in_specs=(P("users", None, None), P(("items", "users"), None)),
        out_specs=(P("users", "items"), P("users")),
        check_vma=False,
    )
```

```python
import functools

import jax
import jax.numpy as jnp
from jax import lax
from jax.experimental import pallas as pl
from jax.experimental.pallas import tpu as pltpu
from jax.sharding import PartitionSpec as P

BLOCK = 1024
LANES = 128
MESH = pl.DeviceIdType.MESH


def landed(ref, sem):
    pltpu.make_async_copy(ref, ref, sem).wait()


def peer(z, d, count):
    if count & (count - 1):
        return (z + d) % count
    out, bit = 0, 1
    while bit < count:
        out = out + ((z // bit + d // bit) % 2) * bit
        bit *= 2
    return out


def by_user(top):
    spread = LANES // 8
    lane = lax.broadcasted_iota(jnp.int32, (top.shape[0], LANES), 1)
    out = None
    for t in range(top.shape[1] // LANES):
        v = top[:, t * LANES : (t + 1) * LANES]
        for shift in (1, 2, 4):
            v = jnp.maximum(v, pltpu.roll(v, LANES - shift, 1))
        v = jnp.take_along_axis(v, (lane % spread) * 8, axis=1)
        out = v if out is None else jnp.where(lane // spread == t, v, out)
    return out


def kernel(
    items, users, caps_hbm, bank_hbm, rel_ref, peak_ref,
    own, bank, all_caps, res, table,
    load_sem, send_sem, recv_sem, back_send, back_recv,
):
    i = lax.axis_index("items")
    g = lax.axis_index("users")
    chips = users // 2
    z, c = g // 2, g % 2
    p = 2 * z + 1 - c
    opposite = peer(i, items - 1, items)
    pieces, rows = all_caps.shape[1], all_caps.shape[2]

    load_caps = pltpu.make_async_copy(caps_hbm, own, load_sem.at[0])
    load_caps.start()
    load_bank = pltpu.make_async_copy(bank_hbm, bank, load_sem.at[1])
    load_bank.start()

    barrier = pltpu.get_barrier_semaphore()

    def hello(jj, gg):
        pl.semaphore_signal(
            barrier, inc=1, device_id={"items": jj, "users": gg}, device_id_type=MESH
        )

    def hello_line(d, carry):
        hello(i, 2 * peer(z, d, chips) + c)
        return carry

    lax.fori_loop(1, chips, hello_line, 0, unroll=chips <= 8)
    for d in range(1, items):
        hello((i + d) % items, g)
    hello(i, p)
    pl.semaphore_wait(barrier, chips - 1 + items - 1 + 1)
    load_caps.wait()

    def send(src, dst, recv, jj, gg):
        pltpu.make_async_remote_copy(
            src_ref=src, dst_ref=dst, send_sem=send_sem.at[0], recv_sem=recv,
            device_id={"items": jj, "users": gg}, device_id_type=MESH,
        ).start()

    def send_line(d, carry):
        far = peer(z, chips - d, chips)
        send(own.at[i], all_caps.at[g, i], recv_sem.at[g, i], i, 2 * far + c)
        return carry

    lax.fori_loop(1, chips, send_line, 0, unroll=chips <= 8)
    send(
        own.at[opposite], all_caps.at[g, opposite], recv_sem.at[g, opposite],
        i, 2 * peer(z, 1, chips) + c,
    )
    send(own, all_caps.at[g], recv_sem.at[g, 0], i, p)
    load_bank.wait()

    def block_peak(group):
        score = lax.dot_general(
            bank[...], group.reshape(pieces * rows, group.shape[-1]),
            (((1,), (1,)), ((), ())), preferred_element_type=jnp.float32,
        )
        return jnp.max(score, axis=0, keepdims=True)

    def answer(gg, jj):
        row = ((i - jj + items) % items) * users + g
        pltpu.make_async_remote_copy(
            src_ref=res.at[gg], dst_ref=table.at[row],
            send_sem=back_send.at[0], recv_sem=back_recv.at[0],
            device_id={"items": jj, "users": gg}, device_id_type=MESH,
        ).start()

    table[g] = block_peak(own[...])
    res[g] = table[g]

    def relay(d, carry):
        from_g = 2 * peer(z, d, chips) + c
        piece, sem = all_caps.at[from_g, i], recv_sem.at[from_g, i]
        landed(piece, sem)
        for s in range(1, items - 1):
            send(piece, piece, sem, peer(i, s, items), g)
        pl.when(d > 1)(lambda: send(piece, piece, sem, opposite, g))
        send(piece, piece, sem, i, p)
        return carry

    lax.fori_loop(1, chips, relay, 0, unroll=chips <= 8)
    landed(all_caps.at[p], recv_sem.at[p, 0])
    res[p] = block_peak(all_caps[p])

    def same_core(d, carry):
        from_g = 2 * peer(z, d, chips) + c
        for s in range(1, items):
            q = (i + s) % items
            piece, sem = all_caps.at[from_g, q], recv_sem.at[from_g, q]
            landed(piece, sem)
            send(piece, piece, sem, i, p)
        res[from_g] = block_peak(all_caps[from_g])
        for s in range(items):
            answer(from_g, (i + s) % items)
        return carry

    lax.fori_loop(1, chips, same_core, 0, unroll=chips <= 8)

    def other_core(d, carry):
        from_g = 2 * peer(z, d, chips) + 1 - c
        for q in range(items):
            landed(all_caps.at[from_g, q], recv_sem.at[from_g, q])
        res[from_g] = block_peak(all_caps[from_g])
        for s in range(items):
            answer(from_g, (i + s) % items)
        return carry

    lax.fori_loop(1, chips, other_core, 0, unroll=chips <= 8)
    for s in range(items):
        answer(p, (i + s) % items)
    for s in range(1, items):
        answer(g, (i + s) % items)

    blocks = items * users
    landed(table.at[pl.ds(0, blocks - 1)], back_recv.at[0])
    best = jnp.max(table[...], axis=0)
    near = table[:users].reshape(users, best.shape[1])
    both = by_user(jnp.concatenate([near, best], axis=0))[:, : peak_ref.shape[1]]
    rel_ref[...] = both[:users] - both[users:]
    peak_ref[...] = both[users:]

    landed(all_caps.at[pl.ds(0, users - 1)], send_sem.at[0])
    landed(table.at[pl.ds(0, blocks - 1)], back_send.at[0])


def per_device(items, users, capsules, bank):
    users_here, k, width = capsules.shape
    assert items & (items - 1) == 0 and users & (users - 1) == 0 and k == 8 and bank.shape[0] == BLOCK and users_here * k <= 8 * LANES
    rows = users_here * k // items
    blocks = items * users
    relative, peak = pl.pallas_call(
        functools.partial(kernel, items, users),
        out_shape=(
            pltpu.VMEM((users, users_here), jnp.float32),
            pltpu.VMEM((1, users_here), jnp.float32),
        ),
        in_specs=[pl.BlockSpec(memory_space=pltpu.HBM)] * 2,
        out_specs=(pl.BlockSpec(memory_space=pltpu.VMEM),) * 2,
        scratch_shapes=[
            pltpu.VMEM((items, rows, width), capsules.dtype),
            pltpu.VMEM(bank.shape, bank.dtype),
            pltpu.VMEM((users, items, rows, width), capsules.dtype),
            pltpu.VMEM((users, 1, users_here * k), jnp.float32),
            pltpu.VMEM((blocks, 1, users_here * k), jnp.float32),
            pltpu.SemaphoreType.DMA((2,)),
            pltpu.SemaphoreType.DMA((1,)),
            pltpu.SemaphoreType.DMA((users, items)),
            pltpu.SemaphoreType.DMA((1,)),
            pltpu.SemaphoreType.DMA((1,)),
        ],
        compiler_params=pltpu.CompilerParams(
            collective_id=0, has_side_effects=True, vmem_limit_bytes=60 * 2**20
        ),
    )(capsules.reshape(items, rows, width), bank)
    return relative.T, peak.reshape(users_here)


def solution(mesh):
    return jax.shard_map(
        functools.partial(per_device, mesh.shape["items"], mesh.shape["users"]),
        mesh=mesh,
        in_specs=(P("users", None, None), P(("items", "users"), None)),
        out_specs=(P("users", "items"), P("users")),
        check_vma=False,
    )
```

```python
import functools

import jax
import jax.numpy as jnp
from jax import lax
from jax.experimental import pallas as pl
from jax.experimental.pallas import tpu as pltpu
from jax.sharding import PartitionSpec as P

BLOCK = 1024
LANES = 128
MESH = pl.DeviceIdType.MESH


def landed(ref, sem):
    pltpu.make_async_copy(ref, ref, sem).wait()


def peer(z, d, count):
    if count & (count - 1):
        return (z + d) % count
    out, bit = 0, 1
    while bit < count:
        out = out + ((z // bit + d // bit) % 2) * bit
        bit *= 2
    return out


def by_user(top):
    spread = LANES // 8
    lane = lax.broadcasted_iota(jnp.int32, (top.shape[0], LANES), 1)
    out = None
    for t in range(top.shape[1] // LANES):
        v = top[:, t * LANES : (t + 1) * LANES]
        for shift in (1, 2, 4):
            v = jnp.maximum(v, pltpu.roll(v, LANES - shift, 1))
        v = jnp.take_along_axis(v, (lane % spread) * 8, axis=1)
        out = v if out is None else jnp.where(lane // spread == t, v, out)
    return out


def kernel(
    items, users, caps_hbm, bank_hbm, rel_ref, peak_ref,
    own, bank, all_caps, res, table,
    load_sem, send_sem, recv_sem, back_send, back_recv,
):
    i = lax.axis_index("items")
    g = lax.axis_index("users")
    chips = users // 2
    z, c = g // 2, g % 2
    p = 2 * z + 1 - c
    opposite = peer(i, items - 1, items)
    pieces, rows = all_caps.shape[1], all_caps.shape[2]

    load_caps = pltpu.make_async_copy(caps_hbm, own, load_sem.at[0])
    load_caps.start()
    load_bank = pltpu.make_async_copy(bank_hbm, bank, load_sem.at[1])
    load_bank.start()

    barrier = pltpu.get_barrier_semaphore()

    def hello(jj, gg):
        pl.semaphore_signal(
            barrier, inc=1, device_id={"items": jj, "users": gg}, device_id_type=MESH
        )

    def hello_line(d, carry):
        hello(i, 2 * peer(z, d, chips) + c)
        return carry

    lax.fori_loop(1, chips, hello_line, 0, unroll=chips <= 8)
    for d in range(1, items):
        hello((i + d) % items, g)
    hello(i, p)
    pl.semaphore_wait(barrier, chips - 1 + items - 1 + 1)
    load_caps.wait()

    def send(src, dst, recv, jj, gg):
        pltpu.make_async_remote_copy(
            src_ref=src, dst_ref=dst, send_sem=send_sem.at[0], recv_sem=recv,
            device_id={"items": jj, "users": gg}, device_id_type=MESH,
        ).start()

    def send_line(d, carry):
        far = peer(z, chips - d, chips)
        send(own.at[i], all_caps.at[g, i], recv_sem.at[g, i], i, 2 * far + c)
        return carry

    lax.fori_loop(1, chips, send_line, 0, unroll=chips <= 8)
    send(
        own.at[opposite], all_caps.at[g, opposite], recv_sem.at[g, opposite],
        i, 2 * peer(z, 1, chips) + c,
    )
    send(own, all_caps.at[g], recv_sem.at[g, 0], i, p)
    load_bank.wait()

    def block_peak(group):
        score = lax.dot_general(
            bank[...], group.reshape(pieces * rows, group.shape[-1]),
            (((1,), (1,)), ((), ())), preferred_element_type=jnp.float32,
        )
        return jnp.max(score, axis=0, keepdims=True)

    def answer(gg, jj):
        row = ((i - jj + items) % items) * users + g
        pltpu.make_async_remote_copy(
            src_ref=res.at[gg], dst_ref=table.at[row],
            send_sem=back_send.at[0], recv_sem=back_recv.at[0],
            device_id={"items": jj, "users": gg}, device_id_type=MESH,
        ).start()

    table[g] = block_peak(own[...])
    res[g] = table[g]

    def relay(d, carry):
        from_g = 2 * peer(z, d, chips) + c
        piece, sem = all_caps.at[from_g, i], recv_sem.at[from_g, i]
        landed(piece, sem)
        for s in range(1, items - 1):
            send(piece, piece, sem, peer(i, s, items), g)
        pl.when(d > 1)(lambda: send(piece, piece, sem, opposite, g))
        send(piece, piece, sem, i, p)
        return carry

    lax.fori_loop(1, chips, relay, 0, unroll=chips <= 8)
    landed(all_caps.at[p], recv_sem.at[p, 0])
    res[p] = block_peak(all_caps[p])

    def same_core(d, carry):
        from_g = 2 * peer(z, d, chips) + c
        for s in range(1, items):
            q = (i + s) % items
            piece, sem = all_caps.at[from_g, q], recv_sem.at[from_g, q]
            landed(piece, sem)
            send(piece, piece, sem, i, p)
        res[from_g] = block_peak(all_caps[from_g])
        for s in range(items):
            answer(from_g, (i + s) % items)
        return carry

    lax.fori_loop(1, chips, same_core, 0, unroll=chips <= 8)

    def other_core(d, carry):
        from_g = 2 * peer(z, d, chips) + 1 - c
        for q in range(items):
            landed(all_caps.at[from_g, q], recv_sem.at[from_g, q])
        res[from_g] = block_peak(all_caps[from_g])
        for s in range(items):
            answer(from_g, (i + s) % items)
        return carry

    lax.fori_loop(1, chips, other_core, 0, unroll=chips <= 8)
    for s in range(items):
        answer(p, (i + s) % items)
    for s in range(1, items):
        answer(g, (i + s) % items)

    blocks = items * users
    landed(table.at[pl.ds(0, blocks - 1)], back_recv.at[0])
    best = jnp.max(table[...], axis=0)
    near = table[:users].reshape(users, best.shape[1])
    both = by_user(jnp.concatenate([near, best], axis=0))[:, : peak_ref.shape[1]]
    rel_ref[...] = both[:users] - both[users:]
    peak_ref[...] = both[users:]

    landed(all_caps.at[pl.ds(0, users - 1)], send_sem.at[0])
    landed(table.at[pl.ds(0, blocks - 1)], back_send.at[0])


def put(relative, peak, relative_hbm, peak_hbm, sem):
    first = pltpu.make_async_copy(relative, relative_hbm, sem.at[0])
    second = pltpu.make_async_copy(peak, peak_hbm, sem.at[1])
    first.start()
    second.start()
    first.wait()
    second.wait()


def per_device(items, users, capsules, bank):
    users_here, k, width = capsules.shape
    assert items & (items - 1) == 0 and users & (users - 1) == 0 and k == 8 and bank.shape[0] == BLOCK and users_here * k <= 8 * LANES
    rows = users_here * k // items
    blocks = items * users
    relative, peak = pl.pallas_call(
        functools.partial(kernel, items, users),
        out_shape=(
            pltpu.VMEM((users, users_here), jnp.float32),
            pltpu.VMEM((1, users_here), jnp.float32),
        ),
        in_specs=[pl.BlockSpec(memory_space=pltpu.HBM)] * 2,
        out_specs=(pl.BlockSpec(memory_space=pltpu.VMEM),) * 2,
        scratch_shapes=[
            pltpu.VMEM((items, rows, width), capsules.dtype),
            pltpu.VMEM(bank.shape, bank.dtype),
            pltpu.VMEM((users, items, rows, width), capsules.dtype),
            pltpu.VMEM((users, 1, users_here * k), jnp.float32),
            pltpu.VMEM((blocks, 1, users_here * k), jnp.float32),
            pltpu.SemaphoreType.DMA((2,)),
            pltpu.SemaphoreType.DMA((1,)),
            pltpu.SemaphoreType.DMA((users, items)),
            pltpu.SemaphoreType.DMA((1,)),
            pltpu.SemaphoreType.DMA((1,)),
        ],
        compiler_params=pltpu.CompilerParams(
            collective_id=0, has_side_effects=True, vmem_limit_bytes=60 * 2**20
        ),
    )(capsules.reshape(items, rows, width), bank)
    relative, peak = pl.pallas_call(
        put,
        out_shape=(pltpu.HBM(relative.shape, relative.dtype), pltpu.HBM(peak.shape, peak.dtype)),
        in_specs=[pl.BlockSpec(memory_space=pltpu.VMEM)] * 2,
        out_specs=(pl.BlockSpec(memory_space=pltpu.HBM),) * 2,
        scratch_shapes=[pltpu.SemaphoreType.DMA((2,))],
    )(
        pltpu.with_memory_space_constraint(relative, pltpu.VMEM),
        pltpu.with_memory_space_constraint(peak, pltpu.VMEM),
    )
    return relative.T, peak.reshape(users_here)


def solution(mesh):
    return jax.shard_map(
        functools.partial(per_device, mesh.shape["items"], mesh.shape["users"]),
        mesh=mesh,
        in_specs=(P("users", None, None), P(("items", "users"), None)),
        out_specs=(P("users", "items"), P("users")),
        check_vma=False,
    )
```
